256 devices in a mesh: grid: 2 (over core), px: 16 (over y, x), py: 8 (over z).
Axes of the slice: x: 4, y: 4, z: 8, core: 2. Of those that a mesh axis runs over, the one named last changes fastest.
Arguments:
- residual: float32 [2, 128, 64, 5, 1024], P('grid', 'px', 'py'), may hold values from -3 to 3
- inverses: float32 [2, 128, 64, 25, 1024], P('grid', 'px', 'py'), may hold values from 0 to 1, as said below
- couplings: float32 [2, 128, 64, 4, 1024], P('grid', 'px', 'py'), may hold values from 0.22 to 0.735, as said below
- receptors: int32 [2, 16, 8, 512], P('grid', 'px', 'py'), may hold values from 0 to 65535, as said below
- owners: int32 [2, 16, 8, 512, 1], P('grid', 'px', 'py'), may hold values from 0 to 127; in each aligned block of 512 rows (0 to 511, 512 to 1023, ..., all dimensions but the last counted through in order) at most 8 rows name the same one
- donors: int32 [2, 16, 8, 512, 8], P('grid', 'px', 'py'), may hold values from 0 to 65535
- weights: float32 [2, 16, 8, 512, 8], P('grid', 'px', 'py'), may hold values from 0 to 1, as said below
Outputs:
- update: float32 [2, 128, 64, 5, 1024], P('grid', 'px', 'py')
The draws below stay inside these ranges and needn't reach their ends.
Inputs may be any that keep to these rules, and one draw needn't show every extreme that they name: `receptors`: receptor indices of one device are distinct. `owners`: among the receptors of one device no owner appears more than 8 times, and in every draw some device names one owner exactly 8 times. `weights`: nonnegative; the 8 weights of a receptor sum to 1. `inverses`: all entries nonnegative; off-diagonal entries 0.02 to 0.07; each row of a block sums to 0.94 to 1. `couplings`: a + b and e + f of each cell lie in 0.88 to 0.98, and each coupling is a quarter to three quarters of its pair's sum.
All inputs are finite; a program needn't handle non-finite values.
Results may differ from the reference program's by a relative error of at most 0.0001.
Values sent between devices are 32-bit elements; how exact they have to be, the bound alone decides.
A program may use at most 128 MiB of HBM per device.

```python
import math
import jax
import jax.numpy as jnp
import numpy as np
from jax import lax

COMPS = 5
DONORS = 8
CI = 8
CJ = 8
CK = 1024
R_DEV = 512
GRIDS = 2
BLOCKS_I = 16
BLOCKS_J = 8
NI = 128
NJ = 64
CELLS = 65536
OWNERS = 128
SLOTS = 8


def draw_residual(key, part):
    shape = (GRIDS, NI, NJ, COMPS, CK)
    return jnp.clip(0.5 * jax.random.normal(key, shape, jnp.float32), -3.0, 3.0)


def draw_inverses(key, part):
    first, second = jax.random.split(key)
    shape = (GRIDS, NI, NJ, COMPS, COMPS, CK)
    row_total = jax.random.uniform(first, (GRIDS, NI, NJ, COMPS, 1, CK), jnp.float32, 0.94, 1.0)
    identity = jnp.eye(COMPS, dtype=jnp.float32).reshape(1, 1, 1, COMPS, COMPS, 1)
    offdiag = jax.random.uniform(second, shape, jnp.float32, 0.02, 0.07) * (1.0 - identity)
    diagonal = row_total - jnp.sum(offdiag, axis=4, keepdims=True)
    blocks = offdiag + identity * diagonal
    return blocks.reshape(GRIDS, NI, NJ, COMPS * COMPS, CK)


def draw_couplings(key, part):
    keys = jax.random.split(key, 4)
    shape = (GRIDS, NI, NJ, 1, CK)
    low_total = 0.88
    lower_total = jax.random.uniform(keys[0], shape, jnp.float32, low_total, 0.98)
    upper_total = jax.random.uniform(keys[1], shape, jnp.float32, low_total, 0.98)
    lower_split = jax.random.uniform(keys[2], shape, jnp.float32, 0.25, 0.75)
    upper_split = jax.random.uniform(keys[3], shape, jnp.float32, 0.25, 0.75)
    return jnp.concatenate([lower_total * lower_split, lower_total * (1.0 - lower_split), upper_total * upper_split, upper_total * (1.0 - upper_split)], axis=3)


def draw_weights(key, part):
    shape = (GRIDS, NI // CI, NJ // CJ, R_DEV, DONORS)
    raw_weight = jax.random.uniform(key, shape, jnp.float32, 0.05, 1.0)
    return raw_weight / jnp.sum(raw_weight, axis=-1, keepdims=True)


def draw_receptors(key, part):
    stride = CELLS // R_DEV
    shape = (GRIDS, NI // CI, NJ // CJ, R_DEV)
    offsets = jax.random.randint(key, shape, 0, stride, dtype=jnp.int32)
    return offsets + jnp.arange(R_DEV, dtype=jnp.int32) * stride


def plant(values, rng, smallest, high):
    index_at = [jax.random.randint(jax.random.fold_in(rng, axis), (), 0, length) for axis, length in enumerate(values.shape)]
    widest = values.shape.index(max(values.shape))
    beside = index_at[:widest] + [(index_at[widest] + 1) % values.shape[widest]] + index_at[widest + 1:]
    return values.at[tuple(index_at)].set(smallest).at[tuple(beside)].set(high)


def deal_out(key, own, number, rows, amount, top, limit, lean):
    order = jax.random.permutation(key, amount)
    heavy_load, common = load_shares(amount, rows * top, limit, lean, True), load_shares(amount, rows * top, limit, lean, False)
    places = jnp.arange(amount)

    def named(tallies, offset_by):
        used = int((tallies > 0).sum())
        fixed = max(1, used // 4)
        shifted = fixed + (places - fixed + offset_by * (used - fixed)) % max(1, amount - fixed)
        return jnp.zeros((amount,), jnp.int32).at[order[jnp.where(places < fixed, places, shifted)]].set(jnp.asarray(tallies, jnp.int32))

    tallies = jnp.where(number % 4 == 0, named(heavy_load, number // 4), named(common, number - number // 4 - 1))
    mixed = jax.random.permutation(jax.random.fold_in(own, 3), amount)
    donor, taker = mixed[0:amount // 2 * 2:2], mixed[1:amount // 2 * 2:2]
    slack = jnp.minimum(tallies[donor] - 1, limit - tallies[taker]) // 2
    slack = jnp.where((donor == order[0]) | (taker == order[0]) | (tallies[taker] == 0), 0, jnp.maximum(slack, 0))
    shifted = jax.random.randint(jax.random.fold_in(own, 4), (amount // 2,), 0, 1 << 20) % (slack + 1)
    tallies = tallies.at[donor].add(-shifted).at[taker].add(shifted)
    items = jnp.searchsorted(jnp.cumsum(tallies), jnp.arange(rows * top), side="right").astype(jnp.int32)
    listing = items.reshape(top, rows).T
    listing = listing[jax.random.permutation(jax.random.fold_in(own, 1), rows)]
    offset_by = jax.random.randint(jax.random.fold_in(own, 2), (rows, 1), 0, top)
    return jnp.take_along_axis(listing, (jnp.arange(top)[None, :] + offset_by) % top, axis=1)


def load_shares(number_of, total, most, skew, full):
    loads = [(1 << 20) // math.isqrt(standing ** skew) + 1 for standing in range(1, number_of + 1)]
    largest = most if full else min(most, max(-(-total // number_of), total * loads[0] // sum(loads)))
    least = 1 if total - largest >= number_of - 1 else 0
    given, surplus = [largest] + [least] * (number_of - 1), total - largest - least * (number_of - 1)
    while surplus > 0:
        movable = [i for i in range(1, number_of) if given[i] < largest] or [i for i in range(1, number_of) if given[i] < most]
        mass, left = sum([loads[i] for i in movable]), surplus
        for i in movable:
            extra = min(most - given[i], max(1, left * loads[i] // mass), surplus)
            given[i] = given[i] + extra
            surplus = surplus - extra
    return np.array(given)


def setup_inputs(seed: int = 0) -> dict:
    key_list = jax.random.split(jax.random.key(seed), 8)
    residual = draw_residual(jax.random.fold_in(key_list[7], 71), 0)
    inverses = draw_inverses(jax.random.fold_in(key_list[7], 71), 0)
    couplings = draw_couplings(jax.random.fold_in(key_list[7], 71), 0)
    receptors = draw_receptors(jax.random.fold_in(key_list[7], 71), 0)
    owners_keys = jax.random.split(jax.random.fold_in(key_list[4], 1), GRIDS * BLOCKS_I * BLOCKS_J * R_DEV // R_DEV)
    owners_turns = jax.random.permutation(jax.random.fold_in(key_list[4], 3), GRIDS * BLOCKS_I * BLOCKS_J * R_DEV // R_DEV)
    owners = jax.vmap(lambda own, number: deal_out(jax.random.fold_in(key_list[4], 2), own, number, R_DEV, OWNERS, 1, SLOTS, 2))(owners_keys, owners_turns).reshape((GRIDS, BLOCKS_I, BLOCKS_J, R_DEV, 1))
    donors = plant(jax.random.randint(key_list[5], (GRIDS, BLOCKS_I, BLOCKS_J, R_DEV, DONORS), 0, CELLS), jax.random.fold_in(key_list[5], 1), 0, CELLS - 1).astype(jnp.int32)
    weights = draw_weights(jax.random.fold_in(key_list[7], 71), 0)
    return {"residual": residual, "inverses": inverses, "couplings": couplings, "receptors": receptors, "owners": owners, "donors": donors, "weights": weights}


def apply_block(block, vector):
    shaped = block.reshape(block.shape[:-2] + (5, 5, block.shape[-1]))
    return jnp.sum(shaped * vector[..., None, :, :], axis=-2)


def forward_grid(rhs_grid, inverse_grid, coupling_grid):
    def row_step(upper_row, inputs):
        rhs_row, inv_row, coup_row = inputs

        def cell_step(left_value, cell_inputs):
            rhs_cell, inv_cell, coup_cell, upper_cell = cell_inputs
            result = apply_block(inv_cell, rhs_cell + coup_cell[0][None] * upper_cell + coup_cell[1][None] * left_value)
            return result, result

        start = jnp.zeros(rhs_row.shape[1:], jnp.float32)
        _, row_values = lax.scan(cell_step, start, (rhs_row, inv_row, coup_row, upper_row))
        return row_values, row_values

    start_row = jnp.zeros(rhs_grid.shape[1:], jnp.float32)
    _, result = lax.scan(row_step, start_row, (rhs_grid, inverse_grid, coupling_grid))
    return result


def backward_grid(star_grid, inverse_grid, coupling_grid):
    def row_step(lower_row, inputs):
        star_row, inv_row, coup_row = inputs

        def cell_step(right_value, cell_inputs):
            star_cell, inv_cell, coup_cell, lower_cell = cell_inputs
            result = star_cell + apply_block(inv_cell, coup_cell[2][None] * lower_cell + coup_cell[3][None] * right_value)
            return result, result

        start = jnp.zeros(star_row.shape[1:], jnp.float32)
        _, row_values = lax.scan(cell_step, start, (star_row, inv_row, coup_row, lower_row), reverse=True)
        return row_values, row_values

    start_row = jnp.zeros(star_grid.shape[1:], jnp.float32)
    _, result = lax.scan(row_step, start_row, (star_grid, inverse_grid, coupling_grid), reverse=True)
    return result


def reference(residual, inverses, couplings, receptors, owners, donors, weights):
    swept_list = []
    for grid_index in range(GRIDS):
        star = forward_grid(residual[grid_index], inverses[grid_index], couplings[grid_index])
        swept_list.append(backward_grid(star, inverses[grid_index], couplings[grid_index]))
    swept = jnp.stack(swept_list)
    owner_list = owners[..., 0]
    owner_i = owner_list // BLOCKS_J
    owner_j = owner_list % BLOCKS_J
    pencil = donors // CK
    donor_i = owner_i[..., None] * CI + pencil // CJ
    donor_j = owner_j[..., None] * CJ + pencil % CJ
    donor_k = donors % CK
    grid_ids = jnp.arange(GRIDS, dtype=jnp.int32).reshape(GRIDS, 1, 1, 1, 1)
    other_grid = (1 - grid_ids) * jnp.ones_like(donors)
    values = swept[other_grid, donor_i, donor_j, :, donor_k]
    fringe = jnp.sum(values * weights[..., None], axis=-2)
    block_i = jnp.arange(BLOCKS_I, dtype=jnp.int32).reshape(1, BLOCKS_I, 1, 1)
    block_j = jnp.arange(BLOCKS_J, dtype=jnp.int32).reshape(1, 1, BLOCKS_J, 1)
    rec_pencil = receptors // CK
    rec_i = block_i * CI + rec_pencil // CJ
    rec_j = block_j * CJ + rec_pencil % CJ
    rec_k = receptors % CK
    rec_grid = grid_ids[..., 0] * jnp.ones_like(receptors)
    return swept.at[rec_grid, rec_i, rec_j, :, rec_k].set(fringe)
```

```python
import functools

import jax
import jax.numpy as jnp
from jax import lax
from jax.experimental import pallas as pl
from jax.experimental.pallas import tpu as pltpu
from jax.sharding import PartitionSpec as P

MESH = pl.DeviceIdType.MESH
LANES = 128
KB = 8
STEPS = 15
ROWS = 34
SLOTS_I = 22
STEP_ROWS = ROWS * 8
UP, LEFT, DOWN, RIGHT = range(4)


def sweep_kernel(nx, ny, inv_h, res_h, cou_h, out_h, data, star, swept, outs, fin, fout, load_sem, out_sem, send_sem, recv_sem):
    px, py = lax.axis_index("px"), lax.axis_index("py")
    depth = px + py
    deepest = nx + ny - 2
    has_source = {UP: px > 0, LEFT: py > 0, DOWN: px < nx - 1, RIGHT: py < ny - 1}
    has_target = {UP: px < nx - 1, LEFT: py < ny - 1, DOWN: px > 0, RIGHT: py > 0}
    target = {UP: {"px": px + 1}, LEFT: {"py": py + 1}, DOWN: {"px": px - 1}, RIGHT: {"py": py - 1}}

    def lanes(block):
        return pl.ds(pl.multiple_of(block * LANES, LANES), LANES)

    def load_block(block, carry):
        def load_row(row, inner):
            slot = 14 - row
            pltpu.make_async_copy(inv_h.at[row, :, :, lanes(block)], data.at[block, slot, pl.ds(0, 25)], load_sem.at[block]).start()
            pltpu.make_async_copy(res_h.at[row, :, :, lanes(block)], data.at[block, slot, pl.ds(25, 5)], load_sem.at[block]).start()
            pltpu.make_async_copy(cou_h.at[row, :, :, lanes(block)], data.at[block, slot, pl.ds(30, 4)], load_sem.at[block]).start()
            return inner

        return lax.fori_loop(0, 8, load_row, carry)

    lax.fori_loop(0, KB, load_block, 0)

    for kind in range(4):

        @pl.when(jnp.logical_not(has_source[kind]))
        def _(kind=kind):
            fin[kind] = jnp.zeros((KB, 5, 8, LANES), jnp.float32)

    barrier = pltpu.get_barrier_semaphore()
    for kind in range(4):

        @pl.when(has_target[kind])
        def _(kind=kind):
            pl.semaphore_signal(barrier, inc=1, device_id=target[kind], device_id_type=MESH)

    inner_x = jnp.logical_and(px > 0, px < nx - 1)
    inner_y = jnp.logical_and(py > 0, py < ny - 1)
    pl.semaphore_wait(barrier, jnp.where(inner_x, 2, 1) + jnp.where(inner_y, 2, 1))

    flat = data.reshape(KB * SLOTS_I * STEP_ROWS, LANES)
    sub = lax.broadcasted_iota(jnp.int32, (8, LANES), 0)

    def face_copy(kind, block):
        return pltpu.make_async_remote_copy(
            src_ref=fout.at[kind, block],
            dst_ref=fin.at[kind, block],
            send_sem=send_sem.at[kind, block],
            recv_sem=recv_sem.at[kind, block],
            device_id=target[kind],
            device_id_type=MESH,
        )

    def receive(kind, block):
        @pl.when(has_source[kind])
        def _():
            face_copy(kind, block).wait_recv()

    def send(kind, block, values, first, stride):
        for c in range(5):
            fout[kind, block, c] = values[pl.ds(block * (STEPS * 40) + c * 8 + first, 8, stride=stride), :]

        @pl.when(has_target[kind])
        def _():
            face_copy(kind, block).start()

    def entry(block, step, row):
        return flat[pl.ds(block * (SLOTS_I * STEP_ROWS) + (14 - step) * STEP_ROWS + row * 8, 8, stride=STEP_ROWS + 1), :]

    def product(block, step, vector):
        result = []
        for r in range(5):
            terms = [entry(block, step, r * 5 + c) * vector[c] for c in range(5)]
            result.append((terms[0] + terms[1]) + (terms[2] + terms[3]) + terms[4])
        return result

    def at_step(block, step, c):
        return pl.ds(pl.multiple_of(block * (STEPS * 40) + (step * 5 + c) * 8, 8), 8)

    def forward(block):
        pltpu.make_async_copy(data.at[block, pl.ds(7, 8)], data.at[block, pl.ds(7, 8)], load_sem.at[block]).wait()
        receive(UP, block)
        receive(LEFT, block)
        value = [jnp.zeros((8, LANES), jnp.float32)] * 5
        for step in range(STEPS):
            low_i, low_j = entry(block, step, 30), entry(block, step, 31)
            vector = []
            for c in range(5):
                upper = value[c]
                left = pltpu.roll(value[c], 1, 0)
                if step < 8:
                    upper = jnp.where(sub == step, fin[UP, block, c], upper)
                    face = jnp.broadcast_to(fin[LEFT, block, c, pl.ds(step, 1), :], (8, LANES))
                    left = jnp.where(sub == 0, face, left)
                vector.append(entry(block, step, 25 + c) + low_i * upper + low_j * left)
            value = product(block, step, vector)
            for c in range(5):
                star[at_step(block, step, c), :] = value[c]
        send(UP, block, star, 7 * 40, 41)
        send(LEFT, block, star, 7 * 40 + 7, 40)

    def backward(block):
        receive(DOWN, block)
        receive(RIGHT, block)
        value = [jnp.zeros((8, LANES), jnp.float32)] * 5
        for step in reversed(range(STEPS)):
            up_i, up_j = entry(block, step, 32), entry(block, step, 33)
            vector = []
            for c in range(5):
                lower = value[c]
                right = pltpu.roll(value[c], 7, 0)
                if step >= 7:
                    lower = jnp.where(sub == step - 7, fin[DOWN, block, c], lower)
                    face = jnp.broadcast_to(fin[RIGHT, block, c, pl.ds(step - 7, 1), :], (8, LANES))
                    right = jnp.where(sub == 7, face, right)
                vector.append(up_i * lower + up_j * right)
            added = product(block, step, vector)
            value = [star[at_step(block, step, c), :] + added[c] for c in range(5)]
            for c in range(5):
                swept[at_step(block, step, c), :] = value[c]
        send(DOWN, block, swept, 0, 41)
        send(RIGHT, block, swept, 0, 40)
        for row in range(8):
            for c in range(5):
                outs[block, row, c] = swept[pl.ds(block * (STEPS * 40) + (row * 5 + c) * 8, 8, stride=41), :]
        pltpu.make_async_copy(outs.at[block], out_h.at[:, :, :, lanes(block)], out_sem.at[block]).start()

    def turn(number, carry):
        corner = depth == deepest
        forth = jnp.where(corner, lax.rem(number, 2) == 0, number < KB)
        block = jnp.where(corner, number // 2, lax.rem(number, KB))

        @pl.when(forth)
        def _():
            forward(block)

        @pl.when(jnp.logical_not(forth))
        def _():
            backward(block)

        return carry

    lax.fori_loop(0, 2 * KB, turn, 0)

    def finish(block, carry):
        pltpu.make_async_copy(outs.at[block], out_h.at[:, :, :, lanes(block)], out_sem.at[block]).wait()
        for kind in range(4):

            @pl.when(has_target[kind])
            def _(kind=kind):
                face_copy(kind, block).wait_send()

        return carry

    lax.fori_loop(0, KB, finish, 0)


def sweep(nx, ny, inverses, residual, couplings):
    any_space = pl.BlockSpec(memory_space=pl.ANY)
    return pl.pallas_call(
        functools.partial(sweep_kernel, nx, ny),
        out_shape=jax.ShapeDtypeStruct((8, 5, 8, KB * LANES), jnp.float32),
        in_specs=[any_space] * 3,
        out_specs=any_space,
        scratch_shapes=[
            pltpu.VMEM((KB, SLOTS_I, ROWS, 8, LANES), jnp.float32),
            pltpu.VMEM((KB * STEPS * 40, LANES), jnp.float32),
            pltpu.VMEM((KB * STEPS * 40, LANES), jnp.float32),
            pltpu.VMEM((KB, 8, 5, 8, LANES), jnp.float32),
            pltpu.VMEM((4, KB, 5, 8, LANES), jnp.float32),
            pltpu.VMEM((4, KB, 5, 8, LANES), jnp.float32),
            pltpu.SemaphoreType.DMA((KB,)),
            pltpu.SemaphoreType.DMA((KB,)),
            pltpu.SemaphoreType.DMA((4, KB)),
            pltpu.SemaphoreType.DMA((4, KB)),
        ],
        compiler_params=pltpu.CompilerParams(collective_id=0, has_side_effects=True, vmem_limit_bytes=48 << 20),
        name="sweep",
    )(inverses, residual, couplings)


def load_field(swept_h, field, sem):
    for block in range(KB):
        pltpu.make_async_copy(swept_h.at[:, :, :, pl.ds(block * LANES, LANES)], field.at[block], sem.at[block]).start()
    for block in range(KB):
        pltpu.make_async_copy(swept_h.at[:, :, :, pl.ds(block * LANES, LANES)], field.at[block], sem.at[block]).wait()


def cell_rows(start):
    return pl.ds(start, 5, stride=8)


def interpolate_kernel(slots, count, start_ref, table_ref, swept_h, out_ref, field, mask, sem):
    lane = lax.broadcasted_iota(jnp.int32, (8, LANES), 1)

    def build(group, carry):
        rows = pl.ds(pl.multiple_of(group * 8, 8), 8)
        block = table_ref[rows, :]
        for d in range(count):
            place = jnp.broadcast_to(block[:, d : d + 1], (8, LANES)).astype(jnp.int32)
            weight = jnp.broadcast_to(block[:, count + d : count + d + 1], (8, LANES))
            mask[d, rows, :] = jnp.where(lane == place, weight, 0.0)
        return carry

    lax.fori_loop(0, slots // 8, build, 0)
    load_field(swept_h, field, sem)
    flat = field.reshape(KB * 8 * 5 * 8, LANES)
    lane5 = lax.broadcasted_iota(jnp.int32, (5, LANES), 1)

    def gather(group, carry):
        result = jnp.zeros((5, LANES), jnp.float32)
        for unit in range(16):
            slot = group * 16 + unit
            terms = []
            for d in range(count):
                start = start_ref[slot * count + d]
                cells = flat[cell_rows(start), :]
                terms.append(cells * mask[d, pl.ds(slot, 1), :])
            while len(terms) > 1:
                terms = [terms[i] + terms[i + 1] for i in range(0, len(terms), 2)]
            total = jnp.sum(terms[0], axis=1, keepdims=True)
            result = jnp.where(lane5 == unit, total, result)
        out_ref[group] = result
        return carry

    lax.fori_loop(0, slots // 16, gather, 0)


def interpolate(start, table, swept):
    slots = table.shape[0]
    count = start.shape[0] // slots
    return pl.pallas_call(
        functools.partial(interpolate_kernel, slots, count),
        out_shape=jax.ShapeDtypeStruct((slots // 16, 5, LANES), jnp.float32),
        in_specs=[
            pl.BlockSpec(memory_space=pltpu.SMEM),
            pl.BlockSpec(memory_space=pltpu.VMEM),
            pl.BlockSpec(memory_space=pl.ANY),
        ],
        out_specs=pl.BlockSpec(memory_space=pltpu.VMEM),
        scratch_shapes=[
            pltpu.VMEM((KB, 8, 5, 8, LANES), jnp.float32),
            pltpu.VMEM((count, slots, LANES), jnp.float32),
            pltpu.SemaphoreType.DMA((KB,)),
        ],
        compiler_params=pltpu.CompilerParams(vmem_limit_bytes=24 << 20),
        name="interpolate",
    )(start, table, swept)


def refresh_kernel(receptors, start_ref, shift_ref, lane_ref, group_ref, value_ref, swept_h, out_h, field, sem, out_sem):
    load_field(swept_h, field, sem)
    flat = field.reshape(KB * 8 * 5 * 8, LANES)
    lane = lax.broadcasted_iota(jnp.int32, (8, LANES), 1)

    def place(batch, carry):
        for unit in range(8):
            r = batch * 8 + unit
            rows = cell_rows(start_ref[r])
            moved = pltpu.roll(value_ref[group_ref[r]], shift_ref[r], 1)
            old = flat[rows, :]
            flat[rows, :] = jnp.where(lane[:5] == lane_ref[r], moved[:5], old)
        return carry

    lax.fori_loop(0, receptors // 8, place, 0)
    for block in range(KB):
        pltpu.make_async_copy(field.at[block], out_h.at[:, :, :, pl.ds(block * LANES, LANES)], out_sem.at[block]).start()
    for block in range(KB):
        pltpu.make_async_copy(field.at[block], out_h.at[:, :, :, pl.ds(block * LANES, LANES)], out_sem.at[block]).wait()


def refresh(start, shift, lane, group, values, swept):
    smem = pl.BlockSpec(memory_space=pltpu.SMEM)
    return pl.pallas_call(
        functools.partial(refresh_kernel, start.shape[0]),
        out_shape=jax.ShapeDtypeStruct(swept.shape, jnp.float32),
        in_specs=[smem] * 4 + [pl.BlockSpec(memory_space=pltpu.VMEM), pl.BlockSpec(memory_space=pl.ANY)],
        out_specs=pl.BlockSpec(memory_space=pl.ANY),
        scratch_shapes=[
            pltpu.VMEM((KB, 8, 5, 8, LANES), jnp.float32),
            pltpu.SemaphoreType.DMA((KB,)),
            pltpu.SemaphoreType.DMA((KB,)),
        ],
        compiler_params=pltpu.CompilerParams(vmem_limit_bytes=16 << 20),
        name="refresh",
    )(start, shift, lane, group, values, swept)


def swapped(array, axis, distance):
    return lax.ppermute(array, axis, [(i, i ^ 1 << distance) for i in range(lax.axis_size(axis))])


def cell_start(cell):
    pencil, k = cell // 1024, cell % 1024
    return (k // LANES * 8 + pencil // 8) * 40 + pencil % 8


def local(residual, inverses, couplings, receptors, owners, donors, weights):
    nx, ny = lax.axis_size("px"), lax.axis_size("py")
    by_row = lambda a: jnp.transpose(a[0], (0, 2, 1, 3))
    receptor_list = receptors[0, 0, 0]
    owner_list = owners[0, 0, 0, :, 0]
    donor_list = donors[0, 0, 0]
    weight_list = weights[0, 0, 0]
    receptor_count, count = donor_list.shape
    owner_count = nx * ny
    slot_count = max(2, 2 * receptor_count // owner_count)
    slots = owner_count * slot_count
    onehot = (owner_list[:, None] == jnp.arange(owner_count, dtype=jnp.int32)[None, :]).astype(jnp.int32)
    slot_rank = jnp.sum((jnp.cumsum(onehot, axis=0) - 1) * onehot, axis=1)
    slot_place = owner_list * slot_count + slot_rank
    asked = jnp.concatenate([donor_list.astype(jnp.float32), weight_list], axis=1)
    request = jnp.zeros((slots, 2 * count), jnp.float32).at[slot_place].set(asked)
    request = swapped(request.reshape(owner_count, slot_count * 2 * count), "grid", 0)
    request = lax.all_to_all(request, ("px", "py"), split_axis=0, concat_axis=0, tiled=True)
    request = request.reshape(slots, 2 * count)
    cell = request[:, :count].astype(jnp.int32)
    table = jnp.concatenate([(cell % LANES).astype(jnp.float32), request[:, count:]], axis=1)
    table = jnp.pad(table, ((0, 0), (0, LANES - 2 * count)))

    swept = sweep(nx, ny, by_row(inverses), by_row(residual), by_row(couplings))

    answer = interpolate(cell_start(cell).reshape(slots * count), table, swept)
    answer = jnp.transpose(answer[:, :, :16], (0, 2, 1)).reshape(owner_count, slot_count * 5)
    answer = lax.all_to_all(answer, ("px", "py"), split_axis=0, concat_axis=0, tiled=True)
    answer = swapped(answer, "grid", 0)
    groups = slots // LANES
    values = jnp.transpose(answer.reshape(groups, LANES, 5), (0, 2, 1))
    values = jnp.pad(values, ((0, 0), (0, 3), (0, 0)))
    lane = receptor_list % LANES
    shift = (lane - slot_place) % LANES
    update = refresh(cell_start(receptor_list), shift, lane, slot_place // LANES, values, swept)
    return jnp.transpose(update, (0, 2, 1, 3))[None]


def solution(mesh):
    placed = (
        P("grid", "px", "py", None, None),
        P("grid", "px", "py", None, None),
        P("grid", "px", "py", None, None),
        P("grid", "px", "py", None),
        P("grid", "px", "py", None, None),
        P("grid", "px", "py", None, None),
        P("grid", "px", "py", None, None),
    )
    return jax.shard_map(
        local,
        mesh=mesh,
        in_specs=placed,
        out_specs=P("grid", "px", "py", None, None),
        check_vma=False,
    )
```
